8 devices in a mesh: datb: 2 (over z, y), model: 2 (over x), data: 2 (over core).
Axes of the slice: x: 2, y: 2, z: 1, core: 2. Of those that a mesh axis runs over, the one named last changes fastest.
Arguments:
- tokens: bfloat16 [4096, 2048], P(('datb', 'data', 'model'))
- w_gate: bfloat16 [2048, 8192], P(('datb', 'data'), 'model')
- w_up: bfloat16 [2048, 8192], P(('datb', 'data'), 'model')
- w_down: bfloat16 [8192, 2048], P('model', ('datb', 'data'))
- grad_out: bfloat16 [4096, 2048], P(('datb', 'data', 'model'))
Outputs:
- output 1: bfloat16 [4096, 2048], P(('datb', 'data', 'model'))
- output 2: bfloat16 [4096, 2048], P(('datb', 'data', 'model'))
- output 3: float32 [2048, 8192], P(('datb', 'data'), 'model')
- output 4: float32 [2048, 8192], P(('datb', 'data'), 'model')
- output 5: float32 [8192, 2048], P('model', ('datb', 'data'))
All inputs are finite; a program needn't handle non-finite values.
Results may differ from the reference program's by a relative error of at most 0.0160102.
Values are sent between devices in bfloat16 or wider.
A program may use at most 1 GiB of HBM per device.

```python
import jax
import jax.numpy as jnp
from jax import lax

D_MODEL = 2048
D_FF = 8192
TOKENS = 4096
BLOCK_ROWS = 512


def setup_inputs(seed: int = 0) -> dict:
    key = jax.random.key(seed)
    k_tok, k_gate, k_up, k_down, k_grad = jax.random.split(key, 5)
    tokens = jax.random.normal(k_tok, (TOKENS, D_MODEL), jnp.float32)
    w_gate = jax.random.normal(k_gate, (D_MODEL, D_FF), jnp.float32) * (D_MODEL ** -0.5)
    w_up = jax.random.normal(k_up, (D_MODEL, D_FF), jnp.float32) * (D_MODEL ** -0.5)
    w_down = jax.random.normal(k_down, (D_FF, D_MODEL), jnp.float32) * (1.5 * D_FF ** -0.5)
    grad_out = jax.random.normal(k_grad, (TOKENS, D_MODEL), jnp.float32)
    return {"tokens": tokens.astype(jnp.bfloat16), "w_gate": w_gate.astype(jnp.bfloat16), "w_up": w_up.astype(jnp.bfloat16), "w_down": w_down.astype(jnp.bfloat16), "grad_out": grad_out.astype(jnp.bfloat16)}


def block_pass(tok_rows, grad_rows, w_gate, w_up, w_down):
    gate_pre = jnp.dot(tok_rows, w_gate, preferred_element_type=jnp.float32).astype(jnp.bfloat16).astype(jnp.float32)
    up_pre = jnp.dot(tok_rows, w_up, preferred_element_type=jnp.float32).astype(jnp.bfloat16).astype(jnp.float32)
    gate_sig = jax.nn.sigmoid(gate_pre)
    silu_gate = gate_pre * gate_sig
    hidden = (silu_gate * up_pre).astype(jnp.bfloat16)
    down_out = jnp.dot(hidden, w_down, preferred_element_type=jnp.float32)
    out_rows = (tok_rows.astype(jnp.float32) + down_out).astype(jnp.bfloat16)
    grad_hidden = jnp.dot(grad_rows, w_down.T, preferred_element_type=jnp.float32).astype(jnp.bfloat16).astype(jnp.float32)
    grad_gate_pre = (grad_hidden * up_pre * gate_sig * (1.0 + gate_pre * (1.0 - gate_sig))).astype(jnp.bfloat16)
    grad_up_pre = (grad_hidden * silu_gate).astype(jnp.bfloat16)
    back_sum = jnp.dot(grad_gate_pre, w_gate.T, preferred_element_type=jnp.float32) + jnp.dot(grad_up_pre, w_up.T, preferred_element_type=jnp.float32)
    grad_in = (grad_rows.astype(jnp.float32) + back_sum).astype(jnp.bfloat16)
    part_gate = jnp.dot(tok_rows.T, grad_gate_pre, preferred_element_type=jnp.float32)
    part_up = jnp.dot(tok_rows.T, grad_up_pre, preferred_element_type=jnp.float32)
    part_down = jnp.dot(hidden.T, grad_rows, preferred_element_type=jnp.float32)
    return out_rows, grad_in, part_gate, part_up, part_down


def reference(tokens, w_gate, w_up, w_down, grad_out):
    block_count = TOKENS // BLOCK_ROWS
    tok_blocks = tokens.reshape(block_count, BLOCK_ROWS, D_MODEL)
    grad_blocks = grad_out.reshape(block_count, BLOCK_ROWS, D_MODEL)

    def scan_step(acc_carry, block_pair):
        acc_gate, acc_up, acc_down = acc_carry
        tok_rows, grad_rows = block_pair
        out_rows, grad_in, part_gate, part_up, part_down = block_pass(tok_rows, grad_rows, w_gate, w_up, w_down)
        return (acc_gate + part_gate, acc_up + part_up, acc_down + part_down), (out_rows, grad_in)

    zero_acc = (jnp.zeros((D_MODEL, D_FF), jnp.float32), jnp.zeros((D_MODEL, D_FF), jnp.float32), jnp.zeros((D_FF, D_MODEL), jnp.float32))
    acc_final, row_outs = lax.scan(scan_step, zero_acc, (tok_blocks, grad_blocks))
    grad_gate, grad_up, grad_down = acc_final
    out_blocks, grad_in_blocks = row_outs
    return (out_blocks.reshape(TOKENS, D_MODEL), grad_in_blocks.reshape(TOKENS, D_MODEL), grad_gate, grad_up, grad_down)
```

```python
import functools

import jax
import jax.numpy as jnp
from jax import lax
from jax.experimental import pallas as pl
from jax.experimental.pallas import tpu as pltpu
from jax.sharding import PartitionSpec as P


ROW_SPEC = P(("datb", "data", "model"), None)
GATE_SPEC = P(("datb", "data"), "model")
DOWN_SPEC = P("model", ("datb", "data"))
AXES = ("datb", "model", "data")
CHUNKS = 4
OWN_TILE = 256
LIMIT = 62 * 1024 * 1024
bf16, f32 = jnp.bfloat16, jnp.float32
ANY = pl.BlockSpec(memory_space=pl.ANY)


def mm(a, b, ca=1, cb=0):
    return lax.dot_general(a, b, (((ca,), (cb,)), ((), ())), preferred_element_type=f32)


def activations(x, dy, wg, wu, wd):
    a = mm(x, wg).astype(bf16).astype(f32)
    b = mm(x, wu).astype(bf16).astype(f32)
    g = mm(dy, wd, 1, 1).astype(bf16).astype(f32)
    sig = jax.nn.sigmoid(a)
    silu = a * sig
    h = (silu * b).astype(bf16)
    da = (g * b * sig * (1.0 + a * (1.0 - sig))).astype(bf16)
    db = (g * silu).astype(bf16)
    return h, da, db


def own_kernel(first, last, half, *refs):
    x_ref, dy_ref, *refs = refs
    pieces, refs = refs[:4], refs[4:]
    if not first:
        (y_in, dx_in), refs = refs[:2], refs[8:]
    sums, (wg, wu, wd, dg, du, dd) = refs[:-6], refs[-6:]
    part = pieces[0].shape[1]
    r = pl.program_id(0)

    @pl.when(r == 0)
    def _():
        for i, piece in enumerate(pieces):
            wg[0, i * part:(i + 1) * part, :] = piece[0]
            wu[0, i * part:(i + 1) * part, :] = piece[1]
            wd[0, :, i * part:(i + 1) * part] = piece[2]
        dg[...] = jnp.zeros_like(dg)
        du[...] = jnp.zeros_like(du)
        dd[...] = jnp.zeros_like(dd)

    x, dy = x_ref[...], dy_ref[...]
    h, da, db = activations(x, dy, wg[0], wu[0], wd[0])
    y = mm(h, wd[0])
    dx = mm(da, wg[0], 1, 1) + mm(db, wu[0], 1, 1)
    if not first:
        y, dx = y + y_in[...], dx + dx_in[...]
    if last:
        y_keep, dx_keep, y_send, dx_send = sums
        keep = pl.num_programs(0) // 2

        @pl.when(r < keep)
        def _():
            y_keep[...] = y
            dx_keep[...] = dx

        @pl.when(r >= keep)
        def _():
            y_send[...] = y.astype(bf16)
            dx_send[...] = dx.astype(bf16)
    else:
        y_out, dx_out = sums
        y_out[...] = y
        dx_out[...] = dx
    dg[...] += mm(x[:, :half], da, 0, 0)
    du[...] += mm(x[:, :half], db, 0, 0)
    dd[...] += mm(h, dy[:, :half], 0, 0)


def grad_kernel(half, x_ref, dy_ref, wg, wu, wd, dg_in, du_in, dd_in, dg, du, dd):
    @pl.when(pl.program_id(1) == 0)
    def _():
        dg[...] = dg_in[...]
        du[...] = du_in[...]
        dd[...] = dd_in[...]

    x, dy = x_ref[...], dy_ref[...]
    h, da, db = activations(x, dy, wg[0], wu[0], wd[0])
    dg[...] += mm(x[:, :half], da, 0, 0)
    du[...] += mm(x[:, :half], db, 0, 0)
    dd[...] += mm(h, dy[:, :half], 0, 0)


def last_kernel(half, fresh, core, x_ref, dy_ref, wg, wu, wd, dg_in, du_in, dd_in, *refs):
    refs = refs if fresh else refs[3:]
    gate, up, down, gate_send, up_send, down_send = refs
    part = half // 2
    x, dy = x_ref[...], dy_ref[...]
    h, da, db = activations(x, dy, wg[0], wu[0], wd[0])
    dg = dg_in[...] + mm(x[:, :half], da, 0, 0)
    gate[...] = dg[:part]
    gate_send[...] = dg[part:]
    du = du_in[...] + mm(x[:, :half], db, 0, 0)
    up[...] = du[:part]
    up_send[...] = du[part:]
    dd = dd_in[...] + mm(h, dy[:, :half], 0, 0)
    down[...] = dd[:, :part]
    down_send[...] = dd[:, part:]


def gather_kernel(masks, *refs):
    *srcs, out = refs
    part = out.shape[2] // 4
    for n, (src, mask) in enumerate(zip(srcs, masks)):
        for i in range(4):
            out[n, :, (i ^ mask) * part:((i ^ mask) + 1) * part] = src[:, i * part:(i + 1) * part]


def gather_rows(blocks, masks):
    count, (rows, cols) = len(blocks), blocks[0].shape
    tile = 64
    out = pl.pallas_call(
        functools.partial(gather_kernel, masks),
        grid=(rows // tile,),
        in_specs=[pl.BlockSpec((tile, cols), lambda t: (t, 0))] * count,
        out_specs=pl.BlockSpec((count, tile, cols), lambda t: (0, t, 0)),
        out_shape=jax.ShapeDtypeStruct((count, rows, cols), blocks[0].dtype),
        cost_estimate=pl.CostEstimate(flops=1000000, bytes_accessed=2 * count * rows * cols * 2, transcendentals=0),
    )(*blocks)
    return out.reshape(count * rows, cols)


def solution(mesh):
    def flip(value, names):
        mask = sum(4 >> AXES.index(name) for name in names)
        return lax.ppermute(value, AXES, [(i, i ^ mask) for i in range(8)])

    def quarters(value, order):
        part = value.shape[1] // 4
        return jnp.concatenate([value[:, i * part:(i + 1) * part] for i in order], axis=1)

    def local_step(tok, wg, wu, wd, dy):
        rows, d_model = tok.shape
        part = d_model // 4
        half = d_model // 2
        ff = wg.shape[1] // 2
        width = ff // CHUNKS
        core = lax.axis_index("data")
        place = 2 * lax.axis_index("datb") + core
        once = pl.Buffered(1)

        def relative(value):
            return jnp.concatenate([lax.dynamic_slice(value, (0, (place ^ i) * part), (value.shape[0], part)) for i in range(4)], axis=1)

        def pieces(which, j):
            start = which * ff + j * width
            gate = lax.dynamic_slice(wg, (0, start), (part, width))
            up = lax.dynamic_slice(wu, (0, start), (part, width))
            down = lax.dynamic_slice(wd, (start, 0), (width, part))
            return lax.optimization_barrier(jnp.stack([gate, up, down]))

        tok_r, dy_r = lax.optimization_barrier((relative(tok), relative(dy)))
        weights = []
        for j in range(CHUNKS):
            same, other = pieces(core, j), pieces(1 - core, j)
            weights.append((same, flip(other, ["data"]), flip(same, ["datb"]), flip(other, ["datb", "data"])))
        tok_x = flip(tok_r, ["model"])
        dy_x = flip(dy_r, ["model"])
        x_own = gather_rows([tok_r, tok_x, flip(tok_r, ["data"]), flip(tok_x, ["data"])], (0, 0, 1, 1))
        dy_own = gather_rows([dy_r, dy_x, flip(dy_r, ["data"]), flip(dy_x, ["data"])], (0, 0, 1, 1))

        early = rows // 2

        def near_far(direct, crossed):
            blocks, masks = [], []
            for block in (direct, crossed):
                if block is not None:
                    blocks += [block, flip(block, ["data"])]
                    masks += [2, 3]
            return gather_rows(blocks, tuple(masks))

        tok_y = flip(tok_r[:early], ["datb"])
        dy_y = flip(dy_r[:early], ["datb"])
        x_ext = near_far(tok_y, flip(tok_y, ["model"]))
        dy_ext = near_far(dy_y, flip(dy_y, ["model"]))
        late_tok = flip(tok_r[early:], ["datb"])
        late_dy = flip(dy_r[early:], ["datb"])
        late_tok_x = flip(tok_x[early:], ["datb"])
        late_dy_x = flip(dy_x[early:], ["datb"])

        w_shapes = [jax.ShapeDtypeStruct((CHUNKS, d_model, width), bf16)] * 2 + [jax.ShapeDtypeStruct((CHUNKS, width, d_model), bf16)]
        d_shapes = [jax.ShapeDtypeStruct((half, ff), f32)] * 2 + [jax.ShapeDtypeStruct((ff, half), f32)]
        params = pltpu.CompilerParams(vmem_limit_bytes=LIMIT)

        def grow(x_rows, dy_rows, carry, chunks):
            start, tile = chunks[0], 512
            row_block = pl.BlockSpec((tile, d_model), lambda j, r: (r, 0))
            specs = [pl.BlockSpec((1, d_model, width), lambda j, r: (start + j, 0, 0))] * 2 + [pl.BlockSpec((1, width, d_model), lambda j, r: (start + j, 0, 0))]
            d_specs = [pl.BlockSpec((half, width), lambda j, r: (0, start + j))] * 2 + [pl.BlockSpec((width, half), lambda j, r: (start + j, 0))]
            grads = pl.pallas_call(
                functools.partial(grad_kernel, half),
                grid=(len(chunks), x_rows.shape[0] // tile),
                in_specs=[row_block] * 2 + specs + d_specs,
                out_specs=d_specs,
                out_shape=d_shapes,
                input_output_aliases={5 + i: i for i in range(3)},
                compiler_params=params,
                cost_estimate=pl.CostEstimate(flops=9 * x_rows.shape[0] * d_model * width * len(chunks), bytes_accessed=50 << 20, transcendentals=0),
            )(x_rows, dy_rows, *carry)
            return [*carry[:3], *grads]

        own_count = 4 * rows
        keep = own_count // OWN_TILE // 2
        for j in range(CHUNKS):
            first, last = j == 0, j == CHUNKS - 1
            row_block = pl.BlockSpec((OWN_TILE, d_model), lambda r: (r, 0))
            piece_block = pl.BlockSpec((3, part, width), lambda r: (0, 0, 0), pipeline_mode=once)
            carry_specs = [pl.BlockSpec((1, d_model, width), lambda r, j=j: (j, 0, 0), pipeline_mode=once)] * 2 + [pl.BlockSpec((1, width, d_model), lambda r, j=j: (j, 0, 0), pipeline_mode=once)] + [pl.BlockSpec((half, width), lambda r, j=j: (0, j), pipeline_mode=once)] * 2 + [pl.BlockSpec((width, half), lambda r, j=j: (j, 0), pipeline_mode=once)]
            if last:
                sum_specs = [pl.BlockSpec((OWN_TILE, d_model), lambda r: (jnp.minimum(r, keep - 1), 0))] * 2 + [pl.BlockSpec((OWN_TILE, d_model), lambda r: (jnp.maximum(r - keep, 0), 0))] * 2
                sum_shapes = [jax.ShapeDtypeStruct((own_count // 2, d_model), f32)] * 2 + [jax.ShapeDtypeStruct((own_count // 2, d_model), bf16)] * 2
            else:
                sum_specs = [row_block] * 2
                sum_shapes = [jax.ShapeDtypeStruct((own_count, d_model), f32)] * 2
            aliases = {} if first else {8 + i: len(sum_specs) + i for i in range(6)}
            if not first and not last:
                aliases |= {6: 0, 7: 1}
            outs = pl.pallas_call(
                functools.partial(own_kernel, first, last, half),
                grid=(own_count // OWN_TILE,),
                in_specs=[row_block] * 2 + [piece_block] * 4 + ([] if first else [row_block] * 2 + [ANY] * 6),
                out_specs=sum_specs + carry_specs,
                out_shape=sum_shapes + w_shapes + d_shapes,
                input_output_aliases=aliases,
                compiler_params=params,
                cost_estimate=pl.CostEstimate(flops=15 * own_count * d_model * width, bytes_accessed=100 << 20, transcendentals=0),
            )(x_own, dy_own, *weights[j], *([] if first else [*sums, *carry]))
            sums, carry = outs[:len(sum_specs)], list(outs[len(sum_specs):])
            if 0 < j < CHUNKS - 1:
                carry = grow(x_ext, dy_ext, carry, (j - 1,))
        y_keep, dx_keep, y_send, dx_send = sums

        def scatter(kept, sent, residual):
            near = flip(sent, ["data"])
            far_part = lax.optimization_barrier((kept[rows:] + quarters(near[rows:], (1, 0, 3, 2)).astype(f32)).astype(bf16))
            far = flip(far_part, ["model"])
            return relative((residual.astype(f32) + kept[:rows] + quarters(near[:rows], (1, 0, 3, 2)).astype(f32) + far.astype(f32)).astype(bf16))

        out = scatter(y_keep, y_send, tok_r)
        grad_in = scatter(dx_keep, dx_send, dy_r)

        for j in (CHUNKS - 2, CHUNKS - 1):
            carry = grow(x_ext, dy_ext, carry, (j,))
        carry = grow(near_far(late_tok, None), near_far(late_dy, None), carry, tuple(range(CHUNKS)))

        x_rows, dy_rows = near_far(late_tok_x, None), near_far(late_dy_x, None)
        finals, sends = None, []
        group = CHUNKS // 2
        for start in range(0, CHUNKS, group):
            row_block = pl.BlockSpec((512, d_model), lambda j, c: (0, 0))
            w_specs = [pl.BlockSpec((1, d_model, width), lambda j, c, s=start: (s + j, 0, 0))] * 2 + [pl.BlockSpec((1, width, d_model), lambda j, c, s=start: (s + j, 0, 0))]
            d_specs = [pl.BlockSpec((half, width), lambda j, c, s=start: (0, s + j))] * 2 + [pl.BlockSpec((width, half), lambda j, c, s=start: (s + j, 0))]
            f_specs = [pl.BlockSpec((part, width), lambda j, c, s=start: (0, c[0] * CHUNKS + s + j))] * 2 + [pl.BlockSpec((width, part), lambda j, c, s=start: (c[0] * CHUNKS + s + j, 0))]
            s_specs = [pl.BlockSpec((part, width), lambda j, c: (0, j))] * 2 + [pl.BlockSpec((width, part), lambda j, c: (j, 0))]
            fresh = finals is None
            outs = pl.pallas_call(
                functools.partial(last_kernel, half, fresh),
                grid_spec=pltpu.PrefetchScalarGridSpec(
                    num_scalar_prefetch=1,
                    grid=(group,),
                    in_specs=[row_block] * 2 + w_specs + d_specs + ([] if fresh else [ANY] * 3),
                    out_specs=f_specs + s_specs,
                ),
                out_shape=[jax.ShapeDtypeStruct((part, 2 * ff), f32)] * 2 + [jax.ShapeDtypeStruct((2 * ff, part), f32)] + [jax.ShapeDtypeStruct((part, group * width), f32)] * 2 + [jax.ShapeDtypeStruct((group * width, part), f32)],
                input_output_aliases={} if fresh else {9 + i: i for i in range(3)},
                compiler_params=params,
                cost_estimate=pl.CostEstimate(flops=9 * 512 * d_model * width * group, bytes_accessed=50 << 20, transcendentals=0),
            )(core.reshape(1), x_rows, dy_rows, *carry, *([] if fresh else finals))
            finals = outs[:3]
            sends.append([flip(v, ["data"]) for v in outs[3:]])
        grad_gate, grad_up, grad_down = finals
        for n, (got_g, got_u, got_d) in enumerate(sends):
            at = (1 - core) * ff + n * group * width
            grad_gate = lax.dynamic_update_slice(grad_gate, got_g, (0, at))
            grad_up = lax.dynamic_update_slice(grad_up, got_u, (0, at))
            grad_down = lax.dynamic_update_slice(grad_down, got_d, (at, 0))
        return out, grad_in, grad_gate, grad_up, grad_down

    return jax.shard_map(local_step, mesh=mesh, in_specs=(ROW_SPEC, GATE_SPEC, GATE_SPEC, DOWN_SPEC, ROW_SPEC), out_specs=(ROW_SPEC, ROW_SPEC, GATE_SPEC, GATE_SPEC, DOWN_SPEC), check_vma=False)
```

```python
import functools

import jax
import jax.numpy as jnp
from jax import lax
from jax.experimental import pallas as pl
from jax.experimental.pallas import tpu as pltpu
from jax.sharding import PartitionSpec as P


ROW_SPEC = P(("datb", "data", "model"), None)
GATE_SPEC = P(("datb", "data"), "model")
DOWN_SPEC = P("model", ("datb", "data"))
AXES = ("datb", "model", "data")
WIDTHS = (512, 512, 512, 512)
TILE = 512
SPANS = ((0, 1024), (1024, 512), (1536, 512))
LIMIT = 62 * 1024 * 1024
bf16, f32 = jnp.bfloat16, jnp.float32
ANY = pl.BlockSpec(memory_space=pl.ANY)


CHUNKS = len(WIDTHS)


def mm(a, b, ca=1, cb=0):
    return lax.dot_general(a, b, (((ca,), (cb,)), ((), ())), preferred_element_type=f32)


def activations(x, dy, wg, wu, wd):
    a = mm(x, wg).astype(bf16).astype(f32)
    b = mm(x, wu).astype(bf16).astype(f32)
    g = mm(dy, wd, 1, 1).astype(bf16).astype(f32)
    sig = jax.nn.sigmoid(a)
    silu = a * sig
    h = (silu * b).astype(bf16)
    da = (g * b * sig * (1.0 + a * (1.0 - sig))).astype(bf16)
    db = (g * silu).astype(bf16)
    return h, da, db


def add_grads(x, dy, h, da, db, refs, half):
    part = half // 2
    for n in range(2):
        at = slice(n * part, (n + 1) * part)
        gate, up, down = refs[3 * n:3 * n + 3]
        gate[...] += mm(x[:, at], da, 0, 0)
        up[...] += mm(x[:, at], db, 0, 0)
        down[...] += mm(h, dy[:, at], 0, 0)


def own_kernel(half, *refs):
    x_ref, dy_ref, *pieces = refs[:6]
    (h_out, da_out, db_out, wg, wu, wd), grads = refs[-12:-6], refs[-6:]
    part = pieces[0].shape[1]

    @pl.when(pl.program_id(0) == 0)
    def _():
        for i, piece in enumerate(pieces):
            at = slice(i * part, (i + 1) * part)
            wg[at, :] = piece[:part, :]
            wu[at, :] = piece[part:2 * part, :]
            wd[:, at] = piece[2 * part:, :]
        for grad in grads:
            grad[...] = jnp.zeros_like(grad)

    x, dy = x_ref[...], dy_ref[...]
    h, da, db = activations(x, dy, wg[...], wu[...], wd[...])
    h_out[...] = h
    da_out[...] = da
    db_out[...] = db
    add_grads(x, dy, h, da, db, grads, half)


def sum_kernel(down, grown, *refs):
    if down:
        h, wd, *refs = refs
        total = mm(h[...], wd[...])
    else:
        da, db, wg, wu, *refs = refs
        total = mm(da[...], wg[...], 1, 1) + mm(db[...], wu[...], 1, 1)
    if grown:
        total += refs[0][...]
    refs[-1][...] = total.astype(refs[-1].dtype)


def late_kernel(part, xd, xp, dyd, dyp, wg, wu, wd, *refs):
    h_out, da_out, db_out, x_q, dy_q, x_sw, dy_sw, xs, dys = refs[-9:]
    block = xd.shape[0]

    @pl.when(pl.program_id(0) == 0)
    def _():
        for slot, (src_x, src_dy, mask) in enumerate(((xd, dyd, 2), (xp, dyp, 3))):
            rows, swapped = (slice(n * block, (n + 1) * block) for n in (slot, 1 - slot))
            for i in range(4):
                to, at = slice((i ^ mask) * part, ((i ^ mask) + 1) * part), slice(i * part, (i + 1) * part)
                xs[rows, to] = src_x[:, at]
                dys[rows, to] = src_dy[:, at]
            at = slice(mask * part, (mask + 1) * part)
            turned = src_x[:, at].T
            x_q[:, rows] = turned
            dy_q[rows, :] = src_dy[:, at]
            x_sw[:, swapped] = turned
            dy_sw[swapped, :] = src_dy[:, at]

    h, da, db = activations(xs[...], dys[...], wg[...], wu[...], wd[...])
    h_out[...] = h.T
    da_out[...] = da
    db_out[...] = db


def last_kernel(count, where, *refs):
    gate_in, up_in, down_in = refs[5 * count:5 * count + 3]
    gate, up, down = refs[-3:]
    dg, du, dd = gate_in[...], up_in[...], down_in[...]
    for n in range(count):
        x, dy, h, da, db = (ref[...] for ref in refs[5 * n:5 * n + 5])
        dg += mm(x, da)
        du += mm(x, db)
        dd += mm(h, dy)
    gate[...] = dg
    up[...] = du
    down[...] = dd


def pair_kernel(kept, near, out):
    out[...] = (kept[...].astype(f32) + near[...].astype(f32)).astype(bf16)


def join_kernel(where, residual, kept, near, far, out):
    out[...] = (residual[...].astype(f32) + kept[...].astype(f32) + near[...].astype(f32) + far[...].astype(f32)).astype(bf16)


def gather_kernel(masks, *refs):
    *srcs, out = refs
    part = out.shape[2] // 4
    for n, (src, mask) in enumerate(zip(srcs, masks)):
        for i in range(4):
            out[n, :, (i ^ mask) * part:((i ^ mask) + 1) * part] = src[:, i * part:(i + 1) * part]


def gather_rows(blocks, masks):
    count, (rows, cols) = len(blocks), blocks[0].shape
    tile = 128
    out = pl.pallas_call(
        functools.partial(gather_kernel, masks),
        grid=(rows // tile,),
        in_specs=[pl.BlockSpec((tile, cols), lambda t: (t, 0))] * count,
        out_specs=pl.BlockSpec((count, tile, cols), lambda t: (0, t, 0)),
        out_shape=jax.ShapeDtypeStruct((count, rows, cols), blocks[0].dtype),
        cost_estimate=pl.CostEstimate(flops=1000000, bytes_accessed=2 * count * rows * cols * 2, transcendentals=0),
    )(*blocks)
    return out.reshape(count * rows, cols)


def solution(mesh):
    def flip(value, names):
        mask = sum(4 >> AXES.index(name) for name in names)
        return lax.ppermute(value, AXES, [(i, i ^ mask) for i in range(8)])

    def local_step(tok, wg, wu, wd, dy):
        rows, d_model = tok.shape
        part = d_model // 4
        half = d_model // 2
        ff = wg.shape[1] // 2
        starts = [sum(WIDTHS[:j]) for j in range(CHUNKS)]
        core = lax.axis_index("data")
        place = 2 * lax.axis_index("datb") + core
        once = pl.Buffered(1)

        def relative(value):
            return jnp.concatenate([lax.dynamic_slice(value, (0, (place ^ i) * part), (value.shape[0], part)) for i in range(4)], axis=1)

        def pieces(which, j):
            start, width = which * ff + starts[j], WIDTHS[j]
            gate = lax.dynamic_slice(wg, (0, start), (part, width))
            up = lax.dynamic_slice(wu, (0, start), (part, width))
            down = lax.dynamic_slice(wd, (start, 0), (width, part))
            return lax.optimization_barrier(jnp.concatenate([gate, up, down], axis=0))

        tok_r, dy_r = lax.optimization_barrier((relative(tok), relative(dy)))
        weights = []
        for j in range(CHUNKS):
            same, other = pieces(core, j), pieces(1 - core, j)
            weights.append((same, flip(other, ["data"]), flip(same, ["datb"]), flip(other, ["datb", "data"])))
        tok_x = flip(tok_r, ["model"])
        dy_x = flip(dy_r, ["model"])
        x_own = gather_rows([tok_r, tok_x, flip(tok_r, ["data"]), flip(tok_x, ["data"])], (0, 0, 1, 1))
        dy_own = gather_rows([dy_r, dy_x, flip(dy_r, ["data"]), flip(dy_x, ["data"])], (0, 0, 1, 1))

        tok_y = flip(tok_r, ["datb"])
        dy_y = flip(dy_r, ["datb"])
        tok_yx = flip(tok_y, ["model"])
        dy_yx = flip(dy_x, ["datb"])

        act_shapes = [jax.ShapeDtypeStruct((4 * rows, ff), bf16)] * 3
        w_shapes = [jax.ShapeDtypeStruct((d_model, ff), bf16)] * 2 + [jax.ShapeDtypeStruct((ff, d_model), bf16)]
        g_shapes = ([jax.ShapeDtypeStruct((part, ff), f32)] * 2 + [jax.ShapeDtypeStruct((ff, part), f32)]) * 2

        def w_specs(width, at, **mode):
            return [pl.BlockSpec((d_model, width), lambda *g: (0, at(*g)), **mode)] * 2 + [pl.BlockSpec((width, d_model), lambda *g: (at(*g), 0), **mode)]

        def g_specs(width, at, **mode):
            return [pl.BlockSpec((part, width), lambda *g: (0, at(*g)), **mode)] * 2 + [pl.BlockSpec((width, part), lambda *g: (at(*g), 0), **mode)]

        def cost(flops):
            return pl.CostEstimate(flops=flops, bytes_accessed=50 << 20, transcendentals=0)

        params = pltpu.CompilerParams(vmem_limit_bytes=LIMIT)

        def sums(down, first_row, count, span, before, dtype):
            (start, width), skip = span, first_row // TILE
            index = start // width
            act = pl.BlockSpec((TILE, width), lambda r: (r + skip, index))
            row_block = pl.BlockSpec((TILE, d_model), lambda r: (r, 0))
            old_block = pl.BlockSpec((TILE, d_model), lambda r: (r + skip, 0))
            every = w_specs(width, lambda r: index, pipeline_mode=once)
            args, specs = (([acts[0], w_all[2]], [act, every[2]]) if down else ([acts[1], acts[2], w_all[0], w_all[1]], [act] * 2 + every[:2]))
            return pl.pallas_call(
                functools.partial(sum_kernel, down, before is not None),
                grid=(count // TILE,),
                in_specs=specs + ([] if before is None else [old_block]),
                out_specs=row_block,
                out_shape=jax.ShapeDtypeStruct((count, d_model), dtype),
                compiler_params=params,
                cost_estimate=cost((2 if down else 4) * count * d_model * width),
            )(*args, *([] if before is None else [before]))

        own_count = 4 * rows
        carry = None
        y_old = dx_old = None
        for j in range(CHUNKS):
            width, index = WIDTHS[j], starts[j] // WIDTHS[j]
            at = lambda r, index=index: index
            row_block = pl.BlockSpec((TILE, d_model), lambda r: (r, 0))
            act_block = pl.BlockSpec((TILE, width), lambda r, index=index: (r, index))
            piece_block = pl.BlockSpec(weights[j][0].shape, lambda r: (0, 0), pipeline_mode=once)
            carry = pl.pallas_call(
                functools.partial(own_kernel, half),
                grid=(own_count // TILE,),
                in_specs=[row_block] * 2 + [piece_block] * 4 + ([] if carry is None else [ANY] * 12),
                out_specs=[act_block] * 3 + w_specs(width, at, pipeline_mode=once) + g_specs(width, at, pipeline_mode=once) * 2,
                out_shape=act_shapes + w_shapes + g_shapes,
                input_output_aliases={} if carry is None else {6 + i: i for i in range(12)},
                compiler_params=params,
                cost_estimate=cost(9 * own_count * d_model * width),
            )(x_own, dy_own, *weights[j], *([] if carry is None else carry))
            acts, w_all, grads = carry[:3], carry[3:6], carry[6:]
            for span in SPANS[:-1]:
                if sum(span) == starts[j] + width:
                    y_old = sums(True, 0, own_count, span, y_old, f32)
                    dx_old = sums(False, 0, own_count, span, dx_old, f32)

        def scatter(down, before, residual):
            sent = sums(down, 2 * rows, 2 * rows, SPANS[-1], before, bf16)
            kept = sums(down, 0, 2 * rows, SPANS[-1], before, bf16)
            near = flip(sent, ["data"])
            quarter = pl.BlockSpec((rows, part), lambda i: (1, i))
            swapped = pl.BlockSpec((rows, part), lambda i: (1, i + 1 - 2 * (i % 2)))
            far_part = pl.pallas_call(
                pair_kernel,
                grid=(4,),
                in_specs=[quarter, swapped],
                out_specs=pl.BlockSpec((rows, part), lambda i: (0, i)),
                out_shape=jax.ShapeDtypeStruct((rows, d_model), bf16),
                compiler_params=params,
                cost_estimate=cost(1 << 22),
            )(kept, near)
            far = flip(far_part, ["model"])
            block_of = lambda i, c: (0, i)
            place_of = lambda i, c: (0, c[i])
            return pl.pallas_call(
                join_kernel,
                grid_spec=pltpu.PrefetchScalarGridSpec(
                    num_scalar_prefetch=1,
                    grid=(4,),
                    in_specs=[pl.BlockSpec((rows, part), block_of)] * 2 + [pl.BlockSpec((rows, part), lambda i, c: (0, i + 1 - 2 * (i % 2))), pl.BlockSpec((rows, part), block_of)],
                    out_specs=pl.BlockSpec((rows, part), place_of),
                ),
                out_shape=jax.ShapeDtypeStruct((rows, d_model), bf16),
                compiler_params=params,
                cost_estimate=cost(1 << 22),
            )(place ^ jnp.arange(4, dtype=jnp.int32), residual, kept, near, far)

        out = scatter(True, y_old, tok_r)
        grad_in = scatter(False, dx_old, dy_r)

        got = [flip(v, ["data"]) for v in grads[3:]]

        late, late_got, step = [], [], 256
        tok_n, dy_n, tok_xn = flip(tok_y, ["data"]), flip(dy_y, ["data"]), flip(tok_yx, ["data"])
        groups = [(rows, (tok_y, tok_n, dy_y, dy_n)), (rows, (tok_yx, tok_xn, dy_yx, flip(dy_yx, ["data"])))]
        for size, blocks in groups:
            blk = [pl.BlockSpec((size, d_model), lambda j: (0, 0), pipeline_mode=once)] * 4
            outs = pl.pallas_call(
                functools.partial(late_kernel, part),
                grid=(ff // step,),
                in_specs=blk + w_specs(step, lambda j: j),
                out_specs=[pl.BlockSpec((step, 2 * size), lambda j: (j, 0))] + [pl.BlockSpec((2 * size, step), lambda j: (0, j))] * 2 + [pl.BlockSpec((part, 2 * size), lambda j: (0, 0)), pl.BlockSpec((2 * size, part), lambda j: (0, 0))] * 2,
                out_shape=[jax.ShapeDtypeStruct((ff, 2 * size), bf16)] + [jax.ShapeDtypeStruct((2 * size, ff), bf16)] * 2 + [jax.ShapeDtypeStruct((part, 2 * size), bf16), jax.ShapeDtypeStruct((2 * size, part), bf16)] * 2,
                scratch_shapes=[pltpu.VMEM((2 * size, d_model), bf16)] * 2,
                compiler_params=params,
                cost_estimate=cost(6 * 2 * size * d_model * ff),
            )(*blocks, *w_all)
            late.append(outs)
            late_got.append([flip(v, ["data"]) for v in outs[:3]])
        count = len(groups)

        finals = ()
        unit = 256
        units = ff // unit
        stages = [(grads[:3], core, [[*late[k][3:5], *late[k][:3]] for k in range(count)]), (got, 1 - core, [[*late[k][5:7], *late_got[k]] for k in range(count)])]
        for before, side, parts in stages:
            late_specs = []
            for size, _ in groups:
                late_specs += [pl.BlockSpec((part, 2 * size), lambda j, c: (0, 0), pipeline_mode=once), pl.BlockSpec((2 * size, part), lambda j, c: (0, 0), pipeline_mode=once), pl.BlockSpec((unit, 2 * size), lambda j, c: (j, 0))] + [pl.BlockSpec((2 * size, unit), lambda j, c: (0, j))] * 2
            place_at = lambda j, c: c[0] * units + j
            finals = pl.pallas_call(
                functools.partial(last_kernel, count),
                grid_spec=pltpu.PrefetchScalarGridSpec(
                    num_scalar_prefetch=1,
                    grid=(units,),
                    in_specs=late_specs + g_specs(unit, lambda j, c: j) + [ANY] * len(finals),
                    out_specs=g_specs(unit, place_at),
                ),
                out_shape=[jax.ShapeDtypeStruct((part, 2 * ff), f32)] * 2 + [jax.ShapeDtypeStruct((2 * ff, part), f32)],
                input_output_aliases={1 + 5 * count + 3 + i: i for i in range(len(finals))},
                compiler_params=params,
                cost_estimate=cost(6 * 4 * rows * part * ff),
            )(side.reshape(1), *[v for group in parts for v in group], *before, *finals)
        return out, grad_in, *finals

    return jax.shard_map(local_step, mesh=mesh, in_specs=(ROW_SPEC, GATE_SPEC, GATE_SPEC, DOWN_SPEC, ROW_SPEC), out_specs=(ROW_SPEC, ROW_SPEC, GATE_SPEC, GATE_SPEC, DOWN_SPEC), check_vma=False)
```

```python
import functools

import jax
import jax.numpy as jnp
from jax import lax
from jax.experimental import pallas as pl
from jax.experimental.pallas import tpu as pltpu
from jax.sharding import PartitionSpec as P


ROW_SPEC = P(("datb", "data", "model"), None)
GATE_SPEC = P(("datb", "data"), "model")
DOWN_SPEC = P("model", ("datb", "data"))
AXES = ("datb", "model", "data")
WIDTHS = (512, 512, 512, 512)
TILE = 512
SPANS = ((0, 1024), (1024, 512), (1536, 512))
LIMIT = 62 * 1024 * 1024
bf16, f32 = jnp.bfloat16, jnp.float32
ANY = pl.BlockSpec(memory_space=pl.ANY)


CHUNKS = len(WIDTHS)


def mm(a, b, ca=1, cb=0):
    return lax.dot_general(a, b, (((ca,), (cb,)), ((), ())), preferred_element_type=f32)


def gated(a, b, g):
    a, b, g = (v.astype(bf16).astype(f32) for v in (a, b, g))
    sig = jax.nn.sigmoid(a)
    silu = a * sig
    h = (silu * b).astype(bf16)
    da = (g * b * sig * (1.0 + a * (1.0 - sig))).astype(bf16)
    db = (g * silu).astype(bf16)
    return h, da, db


def activations(x, dy, wg, wu, wd):
    return gated(mm(x, wg), mm(x, wu), mm(dy, wd, 1, 1))


def add_grads(x, dy, h, da, db, refs, half):
    part = half // 2
    for n in range(2):
        at = slice(n * part, (n + 1) * part)
        gate, up, down = refs[3 * n:3 * n + 3]
        gate[...] += mm(x[:, at], da, 0, 0)
        up[...] += mm(x[:, at], db, 0, 0)
        down[...] += mm(h, dy[:, at], 0, 0)


def own_kernel(half, *refs):
    x_ref, dy_ref, *pieces = refs[:6]
    (h_out, da_out, db_out, wg, wu, wd), grads = refs[-12:-6], refs[-6:]
    part = pieces[0].shape[1]

    @pl.when(pl.program_id(0) == 0)
    def _():
        for i, piece in enumerate(pieces):
            at = slice(i * part, (i + 1) * part)
            wg[at, :] = piece[:part, :]
            wu[at, :] = piece[part:2 * part, :]
            wd[:, at] = piece[2 * part:, :]
        for grad in grads:
            grad[...] = jnp.zeros_like(grad)

    x, dy = x_ref[...], dy_ref[...]
    h, da, db = activations(x, dy, wg[...], wu[...], wd[...])
    h_out[...] = h
    da_out[...] = da
    db_out[...] = db
    add_grads(x, dy, h, da, db, grads, half)


def sum_kernel(down, grown, *refs):
    if down:
        h, wd, *refs = refs
        total = mm(h[...], wd[...])
    else:
        da, db, wg, wu, *refs = refs
        total = mm(da[...], wg[...], 1, 1) + mm(db[...], wu[...], 1, 1)
    if grown:
        total += refs[0][...]
    refs[-1][...] = total.astype(refs[-1].dtype)


def close_kernel(h, da, db, wg, wu, wd, y_old, dx_old, y_out, dx_out):
    y_out[...] = (mm(h[...], wd[...]) + y_old[...]).astype(bf16)
    dx_out[...] = (mm(da[...], wg[...], 1, 1) + mm(db[...], wu[...], 1, 1) + dx_old[...]).astype(bf16)


def place_rows(direct, near, out):
    block, part = direct.shape[0], direct.shape[1] // 4
    for slot, (src, mask) in enumerate(((direct, 2), (near, 3))):
        for i in range(4):
            out[slot * block:(slot + 1) * block, (i ^ mask) * part:((i ^ mask) + 1) * part] = src[:, i * part:(i + 1) * part]


def gate_up_kernel(xd, xp, wg, wu, a_out, b_out, x_t, xs):
    @pl.when(pl.program_id(0) == 0)
    def _():
        place_rows(xd, xp, xs)

    a_out[...] = mm(xs[...], wg[...]).astype(bf16)
    b_out[...] = mm(xs[...], wu[...]).astype(bf16)
    count = x_t.shape[0]
    x_t[...] = xs[:, pl.ds(pl.multiple_of(pl.program_id(0) * count, count), count)].T


def late_kernel(part, dyd, dyp, wd, a, b, x, h_out, da_out, db_out, x_q, dy_q, x_sw, dy_sw, dys):
    block = dyd.shape[0]

    @pl.when(pl.program_id(0) == 0)
    def _():
        place_rows(dyd, dyp, dys)
        for slot in range(2):
            rows, swapped = (slice(n * block, (n + 1) * block) for n in (slot, 1 - slot))
            x_q[:, rows] = x[:, rows]
            x_sw[:, swapped] = x[:, rows]
            dy_q[rows, :] = dys[rows, :part]
            dy_sw[swapped, :] = dys[rows, :part]

    h, da, db = gated(a[...], b[...], mm(dys[...], wd[...], 1, 1))
    h_out[...] = h.T
    da_out[...] = da
    db_out[...] = db


def last_kernel(count, where, *refs):
    gate_in, up_in, down_in = refs[5 * count:5 * count + 3]
    gate, up, down = refs[-3:]
    dg, du, dd = gate_in[...], up_in[...], down_in[...]
    for n in range(count):
        x, dy, h, da, db = (ref[...] for ref in refs[5 * n:5 * n + 5])
        dg += mm(x, da)
        du += mm(x, db)
        dd += mm(h, dy)
    gate[...] = dg
    up[...] = du
    down[...] = dd


def pair_kernel(kept, near, out):
    out[...] = (kept[...].astype(f32) + near[...].astype(f32)).astype(bf16)


def join_kernel(where, residual, kept, near, far, out):
    out[...] = (residual[...].astype(f32) + kept[...].astype(f32) + near[...].astype(f32) + far[...].astype(f32)).astype(bf16)


def gather_kernel(masks, *refs):
    *srcs, out = refs
    part = out.shape[2] // 4
    for n, (src, mask) in enumerate(zip(srcs, masks)):
        for i in range(4):
            out[n, :, (i ^ mask) * part:((i ^ mask) + 1) * part] = src[:, i * part:(i + 1) * part]


def gather_rows(blocks, masks):
    count, (rows, cols) = len(blocks), blocks[0].shape
    tile = 128
    out = pl.pallas_call(
        functools.partial(gather_kernel, masks),
        grid=(rows // tile,),
        in_specs=[pl.BlockSpec((tile, cols), lambda t: (t, 0))] * count,
        out_specs=pl.BlockSpec((count, tile, cols), lambda t: (0, t, 0)),
        out_shape=jax.ShapeDtypeStruct((count, rows, cols), blocks[0].dtype),
        cost_estimate=pl.CostEstimate(flops=1000000, bytes_accessed=2 * count * rows * cols * 2, transcendentals=0),
    )(*blocks)
    return out.reshape(count * rows, cols)


def solution(mesh):
    def flip(value, names):
        mask = sum(4 >> AXES.index(name) for name in names)
        return lax.ppermute(value, AXES, [(i, i ^ mask) for i in range(8)])

    def local_step(tok, wg, wu, wd, dy):
        rows, d_model = tok.shape
        part = d_model // 4
        half = d_model // 2
        ff = wg.shape[1] // 2
        starts = [sum(WIDTHS[:j]) for j in range(CHUNKS)]
        core = lax.axis_index("data")
        place = 2 * lax.axis_index("datb") + core
        once = pl.Buffered(1)

        def relative(value):
            return jnp.concatenate([lax.dynamic_slice(value, (0, (place ^ i) * part), (value.shape[0], part)) for i in range(4)], axis=1)

        def pieces(which, j):
            start, width = which * ff + starts[j], WIDTHS[j]
            gate = lax.dynamic_slice(wg, (0, start), (part, width))
            up = lax.dynamic_slice(wu, (0, start), (part, width))
            down = lax.dynamic_slice(wd, (start, 0), (width, part))
            return lax.optimization_barrier(jnp.concatenate([gate, up, down], axis=0))

        tok_r, dy_r = lax.optimization_barrier((relative(tok), relative(dy)))
        weights = []
        for j in range(CHUNKS):
            same, other = pieces(core, j), pieces(1 - core, j)
            weights.append((same, flip(other, ["data"]), flip(same, ["datb"]), flip(other, ["datb", "data"])))
        tok_x = flip(tok_r, ["model"])
        dy_x = flip(dy_r, ["model"])
        x_own = gather_rows([tok_r, tok_x, flip(tok_r, ["data"]), flip(tok_x, ["data"])], (0, 0, 1, 1))
        dy_own = gather_rows([dy_r, dy_x, flip(dy_r, ["data"]), flip(dy_x, ["data"])], (0, 0, 1, 1))

        tok_y = flip(tok_r, ["datb"])
        dy_y = flip(dy_r, ["datb"])
        tok_yx = flip(tok_y, ["model"])
        dy_yx = flip(dy_x, ["datb"])

        act_shapes = [jax.ShapeDtypeStruct((4 * rows, ff), bf16)] * 3
        w_shapes = [jax.ShapeDtypeStruct((d_model, ff), bf16)] * 2 + [jax.ShapeDtypeStruct((ff, d_model), bf16)]
        g_shapes = ([jax.ShapeDtypeStruct((part, ff), f32)] * 2 + [jax.ShapeDtypeStruct((ff, part), f32)]) * 2

        def w_specs(width, at, **mode):
            return [pl.BlockSpec((d_model, width), lambda *g: (0, at(*g)), **mode)] * 2 + [pl.BlockSpec((width, d_model), lambda *g: (at(*g), 0), **mode)]

        def g_specs(width, at, **mode):
            return [pl.BlockSpec((part, width), lambda *g: (0, at(*g)), **mode)] * 2 + [pl.BlockSpec((width, part), lambda *g: (at(*g), 0), **mode)]

        def cost(flops):
            return pl.CostEstimate(flops=flops, bytes_accessed=50 << 20, transcendentals=0)

        params = pltpu.CompilerParams(vmem_limit_bytes=LIMIT)

        def sums(down, first_row, count, span, before, dtype):
            (start, width), skip = span, first_row // TILE
            index = start // width
            act = pl.BlockSpec((TILE, width), lambda r: (r + skip, index))
            row_block = pl.BlockSpec((TILE, d_model), lambda r: (r, 0))
            old_block = pl.BlockSpec((TILE, d_model), lambda r: (r + skip, 0))
            every = w_specs(width, lambda r: index, pipeline_mode=once)
            args, specs = (([acts[0], w_all[2]], [act, every[2]]) if down else ([acts[1], acts[2], w_all[0], w_all[1]], [act] * 2 + every[:2]))
            return pl.pallas_call(
                functools.partial(sum_kernel, down, before is not None),
                grid=(count // TILE,),
                in_specs=specs + ([] if before is None else [old_block]),
                out_specs=row_block,
                out_shape=jax.ShapeDtypeStruct((count, d_model), dtype),
                compiler_params=params,
                cost_estimate=cost((2 if down else 4) * count * d_model * width),
            )(*args, *([] if before is None else [before]))

        own_count = 4 * rows
        carry = None
        y_old = dx_old = None
        for j in range(CHUNKS):
            width, index = WIDTHS[j], starts[j] // WIDTHS[j]
            at = lambda r, index=index: index
            row_block = pl.BlockSpec((TILE, d_model), lambda r: (r, 0))
            act_block = pl.BlockSpec((TILE, width), lambda r, index=index: (r, index))
            piece_block = pl.BlockSpec(weights[j][0].shape, lambda r: (0, 0), pipeline_mode=once)
            carry = pl.pallas_call(
                functools.partial(own_kernel, half),
                grid=(own_count // TILE,),
                in_specs=[row_block] * 2 + [piece_block] * 4 + ([] if carry is None else [ANY] * 12),
                out_specs=[act_block] * 3 + w_specs(width, at, pipeline_mode=once) + g_specs(width, at, pipeline_mode=once) * 2,
                out_shape=act_shapes + w_shapes + g_shapes,
                input_output_aliases={} if carry is None else {6 + i: i for i in range(12)},
                compiler_params=params,
                cost_estimate=cost(9 * own_count * d_model * width),
            )(x_own, dy_own, *weights[j], *([] if carry is None else carry))
            acts, w_all, grads = carry[:3], carry[3:6], carry[6:]
            for span in SPANS[:-1]:
                if sum(span) == starts[j] + width:
                    y_old = sums(True, 0, own_count, span, y_old, f32)
                    dx_old = sums(False, 0, own_count, span, dx_old, f32)

        def close(first_row):
            (start, width), skip = SPANS[-1], first_row // TILE
            old_block = pl.BlockSpec((TILE, d_model), lambda r: (r + skip, 0))
            act = pl.BlockSpec((TILE, width), lambda r: (r + skip, start // width))
            row_block = pl.BlockSpec((TILE, d_model), lambda r: (r, 0))
            return pl.pallas_call(
                close_kernel,
                grid=(2 * rows // TILE,),
                in_specs=[act] * 3 + w_specs(width, lambda r: start // width, pipeline_mode=once) + [old_block] * 2,
                out_specs=[row_block] * 2,
                out_shape=[jax.ShapeDtypeStruct((2 * rows, d_model), bf16)] * 2,
                compiler_params=params,
                cost_estimate=cost(6 * 2 * rows * d_model * width),
            )(*acts, *w_all, y_old, dx_old)

        y_send, dx_send = close(2 * rows)
        y_keep, dx_keep = close(0)

        def scatter(kept, sent, residual):
            near = flip(sent, ["data"])
            quarter = pl.BlockSpec((rows, part), lambda i: (1, i))
            swapped = pl.BlockSpec((rows, part), lambda i: (1, i + 1 - 2 * (i % 2)))
            far_part = pl.pallas_call(
                pair_kernel,
                grid=(4,),
                in_specs=[quarter, swapped],
                out_specs=pl.BlockSpec((rows, part), lambda i: (0, i)),
                out_shape=jax.ShapeDtypeStruct((rows, d_model), bf16),
                compiler_params=params,
                cost_estimate=cost(1 << 22),
            )(kept, near)
            far = flip(far_part, ["model"])
            piece = pl.BlockSpec((rows, part), lambda i, c: (0, i))
            return pl.pallas_call(
                join_kernel,
                grid_spec=pltpu.PrefetchScalarGridSpec(
                    num_scalar_prefetch=1,
                    grid=(4,),
                    in_specs=[piece, piece, pl.BlockSpec((rows, part), lambda i, c: (0, i + 1 - 2 * (i % 2))), piece],
                    out_specs=pl.BlockSpec((rows, part), lambda i, c: (0, c[i])),
                ),
                out_shape=jax.ShapeDtypeStruct((rows, d_model), bf16),
                compiler_params=params,
                cost_estimate=cost(1 << 22),
            )(place ^ jnp.arange(4, dtype=jnp.int32), residual, kept, near, far)

        out = scatter(y_keep, y_send, tok_r)
        grad_in = scatter(dx_keep, dx_send, dy_r)

        step = 256
        tok_n, dy_n, tok_xn = flip(tok_y, ["data"]), flip(dy_y, ["data"]), flip(tok_yx, ["data"])

        def column(j):
            return (0, j)

        def fixed(j):
            return (0, 0)

        blk = [pl.BlockSpec((rows, d_model), fixed, pipeline_mode=once)] * 2
        every = w_specs(step, lambda j: j)
        ab_block = pl.BlockSpec((2 * rows, step), column)

        def gate_up(direct, near):
            return pl.pallas_call(
                gate_up_kernel,
                grid=(ff // step,),
                in_specs=blk + every[:2],
                out_specs=[ab_block] * 2 + [pl.BlockSpec((half * step // ff, 2 * rows), lambda j: (j, 0))],
                out_shape=[jax.ShapeDtypeStruct((2 * rows, ff), bf16)] * 2 + [jax.ShapeDtypeStruct((half, 2 * rows), bf16)],
                scratch_shapes=[pltpu.VMEM((2 * rows, d_model), bf16)],
                compiler_params=params,
                cost_estimate=cost(4 * 2 * rows * d_model * ff),
            )(direct, near, *w_all[:2])

        got = [flip(v, ["data"]) for v in grads[3:]]
        late, late_got = [], []
        for x_blk, x_near, dy_blk, dy_near in ((tok_y, tok_n, dy_y, dy_n), (tok_yx, tok_xn, dy_yx, flip(dy_yx, ["data"]))):
            a, b, x_t = gate_up(x_blk, x_near)
            outs = pl.pallas_call(
                functools.partial(late_kernel, part),
                grid=(ff // step,),
                in_specs=blk + every[2:] + [ab_block] * 2 + [pl.BlockSpec((part, 2 * rows), fixed, pipeline_mode=once)],
                out_specs=[pl.BlockSpec((step, 2 * rows), lambda j: (j, 0))] + [ab_block] * 2 + [pl.BlockSpec((part, 2 * rows), fixed), pl.BlockSpec((2 * rows, part), fixed)] * 2,
                out_shape=[jax.ShapeDtypeStruct((ff, 2 * rows), bf16)] + [jax.ShapeDtypeStruct((2 * rows, ff), bf16)] * 2 + [jax.ShapeDtypeStruct((part, 2 * rows), bf16), jax.ShapeDtypeStruct((2 * rows, part), bf16)] * 2,
                scratch_shapes=[pltpu.VMEM((2 * rows, d_model), bf16)],
                compiler_params=params,
                cost_estimate=cost(2 * 2 * rows * d_model * ff),
            )(dy_blk, dy_near, w_all[2], a, b, x_t)
            late.append(outs)
            late_got.append([flip(v, ["data"]) for v in outs[:3]])
        groups = [rows, rows]
        count = len(groups)

        finals = ()
        unit = 256
        units = ff // unit
        stages = [(grads[:3], core, [[*late[k][3:5], *late[k][:3]] for k in range(count)]), (got, 1 - core, [[*late[k][5:7], *late_got[k]] for k in range(count)])]
        for before, side, parts in stages:
            late_specs = []
            for size in groups:
                late_specs += [pl.BlockSpec((part, 2 * size), lambda j, c: (0, 0), pipeline_mode=once), pl.BlockSpec((2 * size, part), lambda j, c: (0, 0), pipeline_mode=once), pl.BlockSpec((unit, 2 * size), lambda j, c: (j, 0))] + [pl.BlockSpec((2 * size, unit), lambda j, c: (0, j))] * 2
            place_at = lambda j, c: c[0] * units + j
            finals = pl.pallas_call(
                functools.partial(last_kernel, count),
                grid_spec=pltpu.PrefetchScalarGridSpec(
                    num_scalar_prefetch=1,
                    grid=(units,),
                    in_specs=late_specs + g_specs(unit, lambda j, c: j) + [ANY] * len(finals),
                    out_specs=g_specs(unit, place_at),
                ),
                out_shape=[jax.ShapeDtypeStruct((part, 2 * ff), f32)] * 2 + [jax.ShapeDtypeStruct((2 * ff, part), f32)],
                input_output_aliases={1 + 5 * count + 3 + i: i for i in range(len(finals))},
                compiler_params=params,
                cost_estimate=cost(6 * 4 * rows * part * ff),
            )(side.reshape(1), *[v for group in parts for v in group], *before, *finals)
        return out, grad_in, *finals

    return jax.shard_map(local_step, mesh=mesh, in_specs=(ROW_SPEC, GATE_SPEC, GATE_SPEC, DOWN_SPEC, ROW_SPEC), out_specs=(ROW_SPEC, ROW_SPEC, GATE_SPEC, GATE_SPEC, DOWN_SPEC), check_vma=False)
```

```python
import functools

import jax
import jax.numpy as jnp
from jax import lax
from jax.experimental import pallas as pl
from jax.experimental.pallas import tpu as pltpu
from jax.sharding import PartitionSpec as P


ROW_SPEC = P(("datb", "data", "model"), None)
GATE_SPEC = P(("datb", "data"), "model")
DOWN_SPEC = P("model", ("datb", "data"))
AXES = ("datb", "model", "data")
WIDTHS = (512, 512, 512, 512)
TILE = 512
SPANS = ((0, 1024), (1024, 512), (1536, 512))
LIMIT = 62 * 1024 * 1024
bf16, f32 = jnp.bfloat16, jnp.float32
ANY = pl.BlockSpec(memory_space=pl.ANY)


CHUNKS = len(WIDTHS)


def mm(a, b, ca=1, cb=0):
    return lax.dot_general(a, b, (((ca,), (cb,)), ((), ())), preferred_element_type=f32)


def gated(a, b, g):
    a, b, g = (v.astype(bf16).astype(f32) for v in (a, b, g))
    sig = jax.nn.sigmoid(a)
    silu = a * sig
    h = (silu * b).astype(bf16)
    da = (g * b * sig * (1.0 + a * (1.0 - sig))).astype(bf16)
    db = (g * silu).astype(bf16)
    return h, da, db


def activations(x, dy, wg, wu, wd):
    return gated(mm(x, wg), mm(x, wu), mm(dy, wd, 1, 1))


def add_grads(x, dy, h, da, db, refs, half):
    part = half // 2
    for n in range(2):
        at = slice(n * part, (n + 1) * part)
        gate, up, down = refs[3 * n:3 * n + 3]
        gate[...] += mm(x[:, at], da, 0, 0)
        up[...] += mm(x[:, at], db, 0, 0)
        down[...] += mm(h, dy[:, at], 0, 0)


def own_kernel(half, *refs):
    x_ref, dy_ref, *pieces = refs[:6]
    (h_out, da_out, db_out, wg, wu, wd), grads = refs[-12:-6], refs[-6:]
    part = pieces[0].shape[1]

    @pl.when(pl.program_id(0) == 0)
    def _():
        for i, piece in enumerate(pieces):
            at = slice(i * part, (i + 1) * part)
            wg[at, :] = piece[:part, :]
            wu[at, :] = piece[part:2 * part, :]
            wd[:, at] = piece[2 * part:, :]
        for grad in grads:
            grad[...] = jnp.zeros_like(grad)

    x, dy = x_ref[...], dy_ref[...]
    h, da, db = activations(x, dy, wg[...], wu[...], wd[...])
    h_out[...] = h
    da_out[...] = da
    db_out[...] = db
    add_grads(x, dy, h, da, db, grads, half)


def sum_kernel(down, grown, *refs):
    if down:
        h, wd, *refs = refs
        total = mm(h[...], wd[...])
    else:
        da, db, wg, wu, *refs = refs
        total = mm(da[...], wg[...], 1, 1) + mm(db[...], wu[...], 1, 1)
    if grown:
        total += refs[0][...]
    refs[-1][...] = total.astype(refs[-1].dtype)


def close_kernel(h, da, db, wg, wu, wd, y_old, dx_old, y_out, dx_out):
    y_out[...] = (mm(h[...], wd[...]) + y_old[...]).astype(bf16)
    dx_out[...] = (mm(da[...], wg[...], 1, 1) + mm(db[...], wu[...], 1, 1) + dx_old[...]).astype(bf16)


def place_rows(direct, near, out):
    block, part = direct.shape[0], direct.shape[1] // 4
    for slot, (src, mask) in enumerate(((direct, 2), (near, 3))):
        for i in range(4):
            out[slot * block:(slot + 1) * block, (i ^ mask) * part:((i ^ mask) + 1) * part] = src[:, i * part:(i + 1) * part]


def gate_up_kernel(xd, xp, wg, wu, a_out, b_out, x_t, xs):
    @pl.when(pl.program_id(0) == 0)
    def _():
        place_rows(xd, xp, xs)

    a_out[...] = mm(xs[...], wg[...]).astype(bf16)
    b_out[...] = mm(xs[...], wu[...]).astype(bf16)
    count = x_t.shape[0]
    x_t[...] = xs[:, pl.ds(pl.multiple_of(pl.program_id(0) * count, count), count)].T


def late_kernel(part, dyd, dyp, wd, a, b, x, h_out, da_out, db_out, x_q, dy_q, x_sw, dy_sw, dys):
    block = dyd.shape[0]

    @pl.when(pl.program_id(0) == 0)
    def _():
        place_rows(dyd, dyp, dys)
        for slot in range(2):
            rows, swapped = (slice(n * block, (n + 1) * block) for n in (slot, 1 - slot))
            x_q[:, rows] = x[:, rows]
            x_sw[:, swapped] = x[:, rows]
            dy_q[rows, :] = dys[rows, :part]
            dy_sw[swapped, :] = dys[rows, :part]

    h, da, db = gated(a[...], b[...], mm(dys[...], wd[...], 1, 1))
    h_out[...] = h
    da_out[...] = da
    db_out[...] = db


def last_kernel(count, where, *refs):
    gate_in, up_in, down_in = refs[5 * count:5 * count + 3]
    gate, up, down = refs[-3:]
    dg, du, dd = gate_in[...], up_in[...], down_in[...]
    for n in range(count):
        x, dy, h, da, db = (ref[...] for ref in refs[5 * n:5 * n + 5])
        dg += mm(x, da)
        du += mm(x, db)
        dd += mm(h, dy, 0, 0)
    gate[...] = dg
    up[...] = du
    down[...] = dd


def pair_kernel(kept, near, out):
    out[...] = (kept[...].astype(f32) + near[...].astype(f32)).astype(bf16)


def join_kernel(where, residual, kept, near, far, out):
    out[...] = (residual[...].astype(f32) + kept[...].astype(f32) + near[...].astype(f32) + far[...].astype(f32)).astype(bf16)


def gather_kernel(masks, *refs):
    *srcs, out = refs
    part = out.shape[2] // 4
    for n, (src, mask) in enumerate(zip(srcs, masks)):
        for i in range(4):
            out[n, :, (i ^ mask) * part:((i ^ mask) + 1) * part] = src[:, i * part:(i + 1) * part]


def gather_rows(blocks, masks):
    count, (rows, cols) = len(blocks), blocks[0].shape
    tile = 128
    out = pl.pallas_call(
        functools.partial(gather_kernel, masks),
        grid=(rows // tile,),
        in_specs=[pl.BlockSpec((tile, cols), lambda t: (t, 0))] * count,
        out_specs=pl.BlockSpec((count, tile, cols), lambda t: (0, t, 0)),
        out_shape=jax.ShapeDtypeStruct((count, rows, cols), blocks[0].dtype),
        cost_estimate=pl.CostEstimate(flops=1000000, bytes_accessed=2 * count * rows * cols * 2, transcendentals=0),
    )(*blocks)
    return out.reshape(count * rows, cols)


def solution(mesh):
    def flip(value, names):
        mask = sum(4 >> AXES.index(name) for name in names)
        return lax.ppermute(value, AXES, [(i, i ^ mask) for i in range(8)])

    def local_step(tok, wg, wu, wd, dy):
        rows, d_model = tok.shape
        part = d_model // 4
        half = d_model // 2
        ff = wg.shape[1] // 2
        starts = [sum(WIDTHS[:j]) for j in range(CHUNKS)]
        core = lax.axis_index("data")
        place = 2 * lax.axis_index("datb") + core
        once = pl.Buffered(1)

        def relative(value):
            return jnp.concatenate([lax.dynamic_slice(value, (0, (place ^ i) * part), (value.shape[0], part)) for i in range(4)], axis=1)

        def pieces(which, j):
            start, width = which * ff + starts[j], WIDTHS[j]
            gate = lax.dynamic_slice(wg, (0, start), (part, width))
            up = lax.dynamic_slice(wu, (0, start), (part, width))
            down = lax.dynamic_slice(wd, (start, 0), (width, part))
            return lax.optimization_barrier(jnp.concatenate([gate, up, down], axis=0))

        tok_r, dy_r = lax.optimization_barrier((relative(tok), relative(dy)))
        weights = []
        for j in range(CHUNKS):
            same, other = pieces(core, j), pieces(1 - core, j)
            weights.append((same, flip(other, ["data"]), flip(same, ["datb"]), flip(other, ["datb", "data"])))
        tok_x = flip(tok_r, ["model"])
        dy_x = flip(dy_r, ["model"])
        x_own = gather_rows([tok_r, tok_x, flip(tok_r, ["data"]), flip(tok_x, ["data"])], (0, 0, 1, 1))
        dy_own = gather_rows([dy_r, dy_x, flip(dy_r, ["data"]), flip(dy_x, ["data"])], (0, 0, 1, 1))

        tok_y = flip(tok_r, ["datb"])
        dy_y = flip(dy_r, ["datb"])
        tok_yx = flip(tok_y, ["model"])
        dy_yx = flip(dy_x, ["datb"])

        act_shapes = [jax.ShapeDtypeStruct((4 * rows, ff), bf16)] * 3
        w_shapes = [jax.ShapeDtypeStruct((d_model, ff), bf16)] * 2 + [jax.ShapeDtypeStruct((ff, d_model), bf16)]
        g_shapes = ([jax.ShapeDtypeStruct((part, ff), f32)] * 2 + [jax.ShapeDtypeStruct((ff, part), f32)]) * 2

        def w_specs(width, at, **mode):
            return [pl.BlockSpec((d_model, width), lambda *g: (0, at(*g)), **mode)] * 2 + [pl.BlockSpec((width, d_model), lambda *g: (at(*g), 0), **mode)]

        def g_specs(width, at, **mode):
            return [pl.BlockSpec((part, width), lambda *g: (0, at(*g)), **mode)] * 2 + [pl.BlockSpec((width, part), lambda *g: (at(*g), 0), **mode)]

        def cost(flops):
            return pl.CostEstimate(flops=flops, bytes_accessed=50 << 20, transcendentals=0)

        params = pltpu.CompilerParams(vmem_limit_bytes=LIMIT)

        def sums(down, first_row, count, span, before, dtype):
            (start, width), skip = span, first_row // TILE
            index = start // width
            act = pl.BlockSpec((TILE, width), lambda r: (r + skip, index))
            row_block = pl.BlockSpec((TILE, d_model), lambda r: (r, 0))
            old_block = pl.BlockSpec((TILE, d_model), lambda r: (r + skip, 0))
            every = w_specs(width, lambda r: index, pipeline_mode=once)
            args, specs = (([acts[0], w_all[2]], [act, every[2]]) if down else ([acts[1], acts[2], w_all[0], w_all[1]], [act] * 2 + every[:2]))
            return pl.pallas_call(
                functools.partial(sum_kernel, down, before is not None),
                grid=(count // TILE,),
                in_specs=specs + ([] if before is None else [old_block]),
                out_specs=row_block,
                out_shape=jax.ShapeDtypeStruct((count, d_model), dtype),
                compiler_params=params,
                cost_estimate=cost((2 if down else 4) * count * d_model * width),
            )(*args, *([] if before is None else [before]))

        own_count = 4 * rows
        carry = None
        y_old = dx_old = None
        for j in range(CHUNKS):
            width, index = WIDTHS[j], starts[j] // WIDTHS[j]
            at = lambda r, index=index: index
            row_block = pl.BlockSpec((TILE, d_model), lambda r: (r, 0))
            act_block = pl.BlockSpec((TILE, width), lambda r, index=index: (r, index))
            piece_block = pl.BlockSpec(weights[j][0].shape, lambda r: (0, 0), pipeline_mode=once)
            carry = pl.pallas_call(
                functools.partial(own_kernel, half),
                grid=(own_count // TILE,),
                in_specs=[row_block] * 2 + [piece_block] * 4 + ([] if carry is None else [ANY] * 12),
                out_specs=[act_block] * 3 + w_specs(width, at, pipeline_mode=once) + g_specs(width, at, pipeline_mode=once) * 2,
                out_shape=act_shapes + w_shapes + g_shapes,
                input_output_aliases={} if carry is None else {6 + i: i for i in range(12)},
                compiler_params=params,
                cost_estimate=cost(9 * own_count * d_model * width),
            )(x_own, dy_own, *weights[j], *([] if carry is None else carry))
            acts, w_all, grads = carry[:3], carry[3:6], carry[6:]
            for span in SPANS[:-1]:
                if sum(span) == starts[j] + width:
                    y_old = sums(True, 0, own_count, span, y_old, f32)
                    dx_old = sums(False, 0, own_count, span, dx_old, f32)

        def close(first_row):
            (start, width), skip = SPANS[-1], first_row // TILE
            old_block = pl.BlockSpec((TILE, d_model), lambda r: (r + skip, 0))
            act = pl.BlockSpec((TILE, width), lambda r: (r + skip, start // width))
            row_block = pl.BlockSpec((TILE, d_model), lambda r: (r, 0))
            return pl.pallas_call(
                close_kernel,
                grid=(2 * rows // TILE,),
                in_specs=[act] * 3 + w_specs(width, lambda r: start // width, pipeline_mode=once) + [old_block] * 2,
                out_specs=[row_block] * 2,
                out_shape=[jax.ShapeDtypeStruct((2 * rows, d_model), bf16)] * 2,
                compiler_params=params,
                cost_estimate=cost(6 * 2 * rows * d_model * width),
            )(*acts, *w_all, y_old, dx_old)

        y_send, dx_send = close(2 * rows)
        y_keep, dx_keep = close(0)

        def scatter(kept, sent, residual):
            near = flip(sent, ["data"])
            quarter = pl.BlockSpec((rows, part), lambda i: (1, i))
            swapped = pl.BlockSpec((rows, part), lambda i: (1, i + 1 - 2 * (i % 2)))
            far_part = pl.pallas_call(
                pair_kernel,
                grid=(4,),
                in_specs=[quarter, swapped],
                out_specs=pl.BlockSpec((rows, part), lambda i: (0, i)),
                out_shape=jax.ShapeDtypeStruct((rows, d_model), bf16),
                compiler_params=params,
                cost_estimate=cost(1 << 22),
            )(kept, near)
            far = flip(far_part, ["model"])
            piece = pl.BlockSpec((rows, part), lambda i, c: (0, i))
            return pl.pallas_call(
                join_kernel,
                grid_spec=pltpu.PrefetchScalarGridSpec(
                    num_scalar_prefetch=1,
                    grid=(4,),
                    in_specs=[piece, piece, pl.BlockSpec((rows, part), lambda i, c: (0, i + 1 - 2 * (i % 2))), piece],
                    out_specs=pl.BlockSpec((rows, part), lambda i, c: (0, c[i])),
                ),
                out_shape=jax.ShapeDtypeStruct((rows, d_model), bf16),
                compiler_params=params,
                cost_estimate=cost(1 << 22),
            )(place ^ jnp.arange(4, dtype=jnp.int32), residual, kept, near, far)

        out = scatter(y_keep, y_send, tok_r)
        grad_in = scatter(dx_keep, dx_send, dy_r)

        step = 256
        tok_n, dy_n, tok_xn = flip(tok_y, ["data"]), flip(dy_y, ["data"]), flip(tok_yx, ["data"])

        def column(j):
            return (0, j)

        def fixed(j):
            return (0, 0)

        blk = [pl.BlockSpec((rows, d_model), fixed, pipeline_mode=once)] * 2
        every = w_specs(step, lambda j: j)
        ab_block = pl.BlockSpec((2 * rows, step), column)

        def gate_up(direct, near):
            return pl.pallas_call(
                gate_up_kernel,
                grid=(ff // step,),
                in_specs=blk + every[:2],
                out_specs=[ab_block] * 2 + [pl.BlockSpec((half * step // ff, 2 * rows), lambda j: (j, 0))],
                out_shape=[jax.ShapeDtypeStruct((2 * rows, ff), bf16)] * 2 + [jax.ShapeDtypeStruct((half, 2 * rows), bf16)],
                scratch_shapes=[pltpu.VMEM((2 * rows, d_model), bf16)],
                compiler_params=params,
                cost_estimate=cost(4 * 2 * rows * d_model * ff),
            )(direct, near, *w_all[:2])

        got = [flip(v, ["data"]) for v in grads[3:]]
        late, late_got = [], []
        for x_blk, x_near, dy_blk, dy_near in ((tok_y, tok_n, dy_y, dy_n), (tok_yx, tok_xn, dy_yx, flip(dy_yx, ["data"]))):
            a, b, x_t = gate_up(x_blk, x_near)
            outs = pl.pallas_call(
                functools.partial(late_kernel, part),
                grid=(ff // step,),
                in_specs=blk + every[2:] + [ab_block] * 2 + [pl.BlockSpec((part, 2 * rows), fixed, pipeline_mode=once)],
                out_specs=[ab_block] * 3 + [pl.BlockSpec((part, 2 * rows), fixed), pl.BlockSpec((2 * rows, part), fixed)] * 2,
                out_shape=[jax.ShapeDtypeStruct((2 * rows, ff), bf16)] * 3 + [jax.ShapeDtypeStruct((part, 2 * rows), bf16), jax.ShapeDtypeStruct((2 * rows, part), bf16)] * 2,
                scratch_shapes=[pltpu.VMEM((2 * rows, d_model), bf16)],
                compiler_params=params,
                cost_estimate=cost(2 * 2 * rows * d_model * ff),
            )(dy_blk, dy_near, w_all[2], a, b, x_t)
            late.append(outs)
            late_got.append([flip(v, ["data"]) for v in outs[:3]])
        groups = [rows, rows]
        count = len(groups)

        finals = ()
        unit = 256
        units = ff // unit
        stages = [(grads[:3], core, [[*late[k][3:5], *late[k][:3]] for k in range(count)]), (got, 1 - core, [[*late[k][5:7], *late_got[k]] for k in range(count)])]
        for before, side, parts in stages:
            late_specs = []
            for size in groups:
                late_specs += [pl.BlockSpec((part, 2 * size), lambda j, c: (0, 0), pipeline_mode=once), pl.BlockSpec((2 * size, part), lambda j, c: (0, 0), pipeline_mode=once), pl.BlockSpec((2 * size, unit), lambda j, c: (0, j))] + [pl.BlockSpec((2 * size, unit), lambda j, c: (0, j))] * 2
            place_at = lambda j, c: c[0] * units + j
            finals = pl.pallas_call(
                functools.partial(last_kernel, count),
                grid_spec=pltpu.PrefetchScalarGridSpec(
                    num_scalar_prefetch=1,
                    grid=(units,),
                    in_specs=late_specs + g_specs(unit, lambda j, c: j) + [ANY] * len(finals),
                    out_specs=g_specs(unit, place_at),
                ),
                out_shape=[jax.ShapeDtypeStruct((part, 2 * ff), f32)] * 2 + [jax.ShapeDtypeStruct((2 * ff, part), f32)],
                input_output_aliases={1 + 5 * count + 3 + i: i for i in range(len(finals))},
                compiler_params=params,
                cost_estimate=cost(6 * 4 * rows * part * ff),
            )(side.reshape(1), *[v for group in parts for v in group], *before, *finals)
        return out, grad_in, *finals

    return jax.shard_map(local_step, mesh=mesh, in_specs=(ROW_SPEC, GATE_SPEC, GATE_SPEC, DOWN_SPEC, ROW_SPEC), out_specs=(ROW_SPEC, ROW_SPEC, GATE_SPEC, GATE_SPEC, DOWN_SPEC), check_vma=False)
```
